32 devices in a mesh: row: 8 (over z, x), col: 4 (over y, core).
Axes of the slice: x: 2, y: 2, z: 4, core: 2. Of those that a mesh axis runs over, the one named last changes fastest.
Arguments:
- tokens: bfloat16 [1024, 8192], P('col', 'row'), may hold values from -6 to 6
- grad_out: bfloat16 [1024, 8192], P('col', 'row'), may hold values from -2 to 2
- gate: bfloat16 [1024, 14336], P('row', 'col'), may hold values from -6 to 6
- up: bfloat16 [1024, 14336], P('row', 'col'), may hold values from -6 to 6
- gate_weight: bfloat16 [8192, 14336], P('row', 'col'), may hold values from -0.0625 to 0.0625
- up_weight: bfloat16 [8192, 14336], P('row', 'col'), may hold values from -0.0625 to 0.0625
- down_weight: bfloat16 [8192, 14336], P('row', 'col'), may hold values from -0.046875 to 0.046875
Outputs:
- grad_tokens: bfloat16 [1024, 8192], P('col', 'row')
- grad_gate_weight: float32 [8192, 14336], P('row', 'col')
- grad_up_weight: float32 [8192, 14336], P('row', 'col')
- grad_down_weight: float32 [8192, 14336], P('row', 'col')
The draws below stay inside these ranges and needn't reach their ends.
All inputs are finite; a program needn't handle non-finite values.
Results may differ from the reference program's by a relative error of at most 0.0049.
Values may be sent and summed in bfloat16 or wider, within the bound.
A program may use at most 192 MiB of HBM per device.

```python
import jax
import jax.numpy as jnp
from jax import lax

D = 8192
FF = 14336
TOKENS = 1024


def raised(result, key, source, target, blocks, factor):
    def block_of(dim):
        return (jnp.arange(result.shape[dim]) // (result.shape[dim] // blocks)).reshape((-1,) + (1,) * (result.ndim - 1 - dim))

    near = jax.random.permutation(key, blocks)[block_of(target)]
    second = (block_of(target) + blocks // 2) % blocks
    return jnp.where((block_of(source) == near) | (block_of(source) == second), factor * result, result)


def block_scale(own_key, shape, pieces, low, high):
    def one(dim, parts):
        draws = jax.random.uniform(jax.random.fold_in(jax.random.fold_in(own_key, 6), dim), (parts,), jnp.float32, low / len(pieces), high / len(pieces))
        return jnp.repeat(jnp.exp(draws), shape[dim] // parts).reshape((-1,) + (1,) * (len(shape) - dim - 1))

    level = one(*pieces[0])
    for cut in pieces[1:]:
        level = level * one(*cut)
    return level


def noise(key, shape, scale, bound, split=(), kind=jnp.bfloat16):
    result = scale * jax.random.normal(key, shape, jnp.float32)
    if split:
        result = result * block_scale(key, shape, split, -0.22, 0.18)
    return jnp.clip(result, -bound, bound).astype(kind)


def bell_draw_with(rng, shape, scale, most, shards, heavy, held_as=jnp.bfloat16):
    array = scale * jax.random.normal(rng, shape, jnp.float32)
    if shards:
        array = array * block_scale(rng, shape, shards, -0.22, 0.18)
    return jnp.clip(raised(array, jax.random.fold_in(rng, 3), *heavy), -most, most).astype(held_as)


def setup_inputs(seed: int = 0) -> dict:
    splits = jax.random.split(jax.random.key(seed), 8)
    tokens = noise(splits[0], (TOKENS, D), 1.0, 6.0, ((0, 4), (1, 8)))
    grad_out = bell_draw_with(splits[1], (TOKENS, D), 0.25, 2.0, ((0, 4), (1, 8)), (1, 0, 8, 2.0))
    gate = noise(splits[2], (TOKENS, FF), 1.0, 6.0, ((0, 8), (1, 4)))
    up = noise(splits[3], (TOKENS, FF), 1.0, 6.0, ((0, 8), (1, 4)))
    gate_weight = noise(splits[4], (D, FF), D ** -0.5, 0.0625, ((0, 8), (1, 4)))
    up_weight = noise(splits[5], (D, FF), D ** -0.5, 0.0625, ((0, 8), (1, 4)))
    down_weight = noise(splits[6], (D, FF), FF ** -0.5, 0.046875, ((0, 8), (1, 4)))
    return {"tokens": tokens, "grad_out": grad_out, "gate": gate, "up": up, "gate_weight": gate_weight, "up_weight": up_weight, "down_weight": down_weight}


def reference(tokens, grad_out, gate, up, gate_weight, up_weight, down_weight):
    gate32 = gate.astype(jnp.float32)
    up32 = up.astype(jnp.float32)
    sigma = jax.nn.sigmoid(gate32)
    active = gate32 * sigma
    hidden = (active * up32).astype(jnp.bfloat16)
    grad_hidden = jnp.dot(grad_out, down_weight, preferred_element_type=jnp.float32)
    grad_up = (grad_hidden * active).astype(jnp.bfloat16)
    grad_gate = (grad_hidden * up32 * sigma * (1.0 + gate32 * (1.0 - sigma))).astype(jnp.bfloat16)
    grad_down_weight = jnp.dot(grad_out.T, hidden, preferred_element_type=jnp.float32)
    grad_gate_weight = jnp.dot(tokens.T, grad_gate, preferred_element_type=jnp.float32)
    grad_up_weight = jnp.dot(tokens.T, grad_up, preferred_element_type=jnp.float32)
    dims = (((1,), (1,)), ((), ()))
    grad_tokens = lax.dot_general(grad_gate, gate_weight, dims, preferred_element_type=jnp.float32)
    grad_tokens = grad_tokens + lax.dot_general(grad_up, up_weight, dims, preferred_element_type=jnp.float32)
    return grad_tokens.astype(jnp.bfloat16), grad_gate_weight, grad_up_weight, grad_down_weight
```

```python
import jax
import jax.numpy as jnp
from jax import lax
from jax.sharding import PartitionSpec as P


def backward_parts(grad_hidden, gate, up):
    gate32 = gate.astype(jnp.float32)
    up32 = up.astype(jnp.float32)
    sigma = jax.nn.sigmoid(gate32)
    grad_up = (grad_hidden * (gate32 * sigma)).astype(jnp.bfloat16)
    grad_gate = (grad_hidden * up32 * sigma * (1.0 + gate32 * (1.0 - sigma))).astype(jnp.bfloat16)
    return grad_gate, grad_up


class Ring:
    def __init__(self, n):
        self.n = n
        self.order = list(range(0, n, 2)) + list(range(1, n, 2))[::-1]
        self.place = [self.order.index(r) for r in range(n)]
        self.up = [(self.order[k], self.order[(k + 1) % n]) for k in range(n)]
        self.down = [(b, a) for a, b in self.up]

    def forward(self, x):
        return lax.ppermute(x, "row", self.up)

    def backward(self, x):
        return lax.ppermute(x, "row", self.down)

    def owners(self):
        mine = jnp.asarray(self.place)[lax.axis_index("row")]
        held = jnp.asarray(self.order)[(mine + jnp.arange(self.n)) % self.n]
        return [held[k] for k in range(self.n)]

    def steps(self, x, ready=lambda step, *pair: pair):
        n = self.n
        ahead = behind = x
        for step in range(1, (n + 1) // 2):
            behind, ahead = ready(step, behind, ahead)
            behind = self.forward(behind)
            ahead = self.backward(ahead)
            yield [(n - step, behind), (step, ahead)]
        if n % 2 == 0:
            half = x.shape[1] // 2
            behind, ahead = ready(n // 2, behind, ahead)
            yield [(n // 2, self.forward(behind[:, :half])), (n // 2, self.backward(ahead[:, half:]))]

    def place_blocks(self, owners, x, arrived):
        size, width = x.shape
        whole = jnp.zeros((self.n * size, width), x.dtype)
        whole = lax.dynamic_update_slice(whole, x, (owners[0] * size, 0))
        for pair in arrived:
            column = 0
            for offset, block in pair:
                start = column if block.shape[1] < width else 0
                whole = lax.dynamic_update_slice(whole, block, (owners[offset] * size, start))
                column += block.shape[1]
        return whole


def after(first, *then):
    return lax.optimization_barrier((first, *then))


def make_per_device(n):
    ring = Ring(n)

    def per_device(tokens, grad_out, gate, up, gate_weight, up_weight, down_weight):
        owners = ring.owners()
        size, width = gate.shape
        half = width // 2
        low = jnp.bfloat16

        gate32 = gate.astype(jnp.float32)
        hidden = (gate32 * jax.nn.sigmoid(gate32) * up.astype(jnp.float32)).astype(low)
        moves = ring.steps(hidden)
        hidden_blocks = []

        def next_hidden(*values):
            step = next(moves, None)
            if step is None:
                return values
            (i, a), (j, b) = step
            a, b, *values = after(a, b, *values)
            hidden_blocks.append([(i, a), (j, b)])
            return values

        grad_all = lax.all_gather(grad_out, "col", axis=0, tiled=True)
        grad_all, tokens = after(grad_all, tokens)
        tokens_all = lax.all_gather(tokens, "col", axis=0, tiled=True)
        partial = jnp.dot(grad_all, down_weight, preferred_element_type=jnp.float32)

        def block(k):
            return lax.dynamic_slice_in_dim(partial, owners[k] * size, size, 0)

        sum_up = sum_down = None
        if n % 2 == 0:
            far = block(n // 2).astype(low)
            send_up, send_down = next_hidden(far[:, :half], far[:, half:])
            sum_up = ring.forward(send_up).astype(jnp.float32)
            sum_down = ring.backward(send_down).astype(jnp.float32)
        for step in range((n - 1) // 2, 0, -1):
            send_up, send_down = block(step), block(n - step)
            if sum_up is not None:
                if sum_up.shape[1] == half:
                    sum_up = jnp.pad(sum_up, ((0, 0), (0, width - half)))
                    sum_down = jnp.pad(sum_down, ((0, 0), (half, 0)))
                send_up = send_up + sum_up
                send_down = send_down + sum_down
            send_up, send_down = next_hidden(send_up.astype(low), send_down.astype(low))
            sum_up = ring.forward(send_up).astype(jnp.float32)
            sum_down = ring.backward(send_down).astype(jnp.float32)
        grad_hidden = block(0) + sum_up + sum_down
        grad_gate, grad_up = backward_parts(grad_hidden, gate, up)

        hidden_blocks.extend(list(moves))
        hidden_all = ring.place_blocks(owners, hidden, hidden_blocks)
        gate_blocks = list(ring.steps(grad_gate))
        gate_all = ring.place_blocks(owners, grad_gate, gate_blocks)
        grad_t, tokens_t = lax.optimization_barrier((grad_all.T, tokens_all.T))
        grad_down_weight = jnp.dot(grad_t, hidden_all, preferred_element_type=jnp.float32)
        grad_gate_weight = jnp.dot(tokens_t, gate_all, preferred_element_type=jnp.float32)
        inner = (((1,), (1,)), ((), ()))
        first = lax.dot_general(gate_all, gate_weight, inner, preferred_element_type=jnp.float32)

        def products_done(step, *pair):
            nonlocal first, grad_gate_weight, grad_down_weight
            if step == 1:
                grad_down_weight, *pair = after(grad_down_weight, *pair)
            if step == n // 2 - 1:
                first, *pair = after(first, *pair)
            if step == n // 2:
                grad_gate_weight, *pair = after(grad_gate_weight, *pair)
            return pair

        last = [block for _, block in gate_blocks[-2 if len(gate_blocks) > 1 else -1]]
        *_, grad_up_sent = after(*last, grad_up)
        up_all = ring.place_blocks(owners, grad_up, list(ring.steps(grad_up_sent, products_done)))
        both = first + lax.dot_general(up_all, up_weight, inner, preferred_element_type=jnp.float32)
        grad_tokens = lax.psum_scatter(both, "col", scatter_dimension=0, tiled=True)
        grad_up_weight = jnp.dot(tokens_t, up_all, preferred_element_type=jnp.float32)
        return (grad_tokens.astype(low), grad_gate_weight, grad_up_weight, grad_down_weight)

    return per_device


def solution(mesh):
    return jax.shard_map(
        make_per_device(mesh.shape["row"]),
        mesh=mesh,
        in_specs=(
            P("col", "row"),
            P("col", "row"),
            P("row", "col"),
            P("row", "col"),
            P("row", "col"),
            P("row", "col"),
            P("row", "col"),
        ),
        out_specs=(P("col", "row"), P("row", "col"), P("row", "col"), P("row", "col")),
        check_vma=False,
    )
```
